32 devices in a mesh: row: 8 (over y, x, core), col: 4 (over z).
Axes of the slice: x: 2, y: 2, z: 4, core: 2. Of those that a mesh axis runs over, the one named last changes fastest.
Arguments:
- choi: float32 [4, 2048, 1024], P(None, 'row', 'col'), may hold values from -0.5 to 8, as said below
Outputs:
- factored: float32 [4, 2048, 1024], P(None, 'row', 'col')
The draws below stay inside these ranges and needn't reach their ends.
Inputs may be any that keep to these rules, and one draw needn't show every extreme that they name: `choi`: the leading 1024 x 1024 block of the matrix is symmetric with a positive diagonal, and its leading 2 * 256 square is positive definite.
All inputs are finite; a program needn't handle non-finite values.
Results may differ from the reference program's by a relative error of at most 0.0001.
Values sent between devices are 32-bit elements; how exact they have to be, the bound alone decides.
A program may use at most 64 MiB of HBM per device.

```python
import math
import jax
import jax.numpy as jnp
from jax import lax

TILE = 256
RT_DEV = 4
PANELS = 2
ORDER = 8192
COLS = 1024
N_ROW = 8


off_spread = 0.04


def draw_choi(key, part):
    first = jax.random.fold_in(key, 11)
    second = jax.random.fold_in(key, 23)
    noise_draw = jax.random.normal(first, (ORDER, COLS), jnp.float32) * off_spread
    diag_draw = jax.random.uniform(second, (COLS,), jnp.float32, 4.5, 8.0)
    upper_part = noise_draw[:COLS]
    symmetric = (upper_part + upper_part.T) * math.sqrt(0.5)
    ident_mask = jnp.arange(COLS)[:, None] == jnp.arange(COLS)[None, :]
    symmetric = jnp.where(ident_mask, diag_draw[:, None], symmetric)
    whole_matrix = jnp.concatenate([symmetric, noise_draw[COLS:]], axis=0)
    return whole_matrix.reshape(RT_DEV, ORDER // RT_DEV, COLS)


def setup_inputs(seed: int = 0) -> dict:
    splits = jax.random.split(jax.random.key(seed), 2)
    return {
        "choi": draw_choi(jax.random.fold_in(splits[1], 71), 0),
    }


def reference(choi):
    matrix = choi.reshape(RT_DEV * N_ROW * TILE, COLS)
    identity = jnp.eye(TILE, dtype=matrix.dtype)
    for step in range(PANELS):
        start = step * TILE
        finish = start + TILE
        factor = jnp.linalg.cholesky(matrix[start:finish, start:finish])
        inverse = jax.scipy.linalg.solve_triangular(factor, identity, lower=True)
        beneath = jnp.dot(matrix[finish:, start:finish], inverse.T, precision=lax.Precision.HIGHEST)
        column = jnp.concatenate([jnp.zeros((start, TILE), matrix.dtype), factor, beneath], axis=0)
        matrix = matrix.at[:, start:finish].set(column)
        change = jnp.dot(beneath, beneath[:COLS - finish].T, precision=lax.Precision.HIGHEST)
        matrix = matrix.at[finish:, finish:].add(-change)
    matrix = matrix.at[:PANELS * TILE, PANELS * TILE:].set(0.0)
    return matrix.reshape(RT_DEV, N_ROW * TILE, COLS)
```

```python
import functools

import jax
import jax.numpy as jnp
from jax import lax
from jax.experimental import pallas as pl
from jax.experimental.pallas import tpu as pltpu
from jax.sharding import PartitionSpec as P

MESH = pl.DeviceIdType.MESH
HIGHEST = lax.Precision.HIGHEST
F32 = jnp.float32

TILES = ((0, 0, 0, 4), (1, 0, 1, 2), (1, 1, 1, 2), (0, None, 2, 2), (1, None, 2, 2))
ARRIVAL = (3, 4, 0, 1, 2)
MAX_CHUNKS = 4


def dot(a, b, ca=1, cb=0, precision=HIGHEST):
    return lax.dot_general(
        a, b, (((ca,), (cb,)), ((), ())), precision=precision, preferred_element_type=F32
    )


def pivot_rows(rows, lane, sub, first):
    n = rows.shape[1]
    wide = [jnp.broadcast_to(rows[j : j + 1, :], (8, n)) for j in range(8)]
    columns = [
        jnp.sum(jnp.where(lane == first + j, rows, 0.0), axis=1, keepdims=True) for j in range(8)
    ]
    columns = [jnp.broadcast_to(c, (8, n)) for c in columns]
    entry = [
        [jnp.broadcast_to(columns[j][i : i + 1, :], (8, n)) if j <= i else None for j in range(8)]
        for i in range(8)
    ]
    final = jnp.zeros((8, n), F32)
    for j in range(8):
        here = lane == first + j
        pivot = entry[j][j]
        inverse = 1.0 / pivot
        base = jnp.where(here, 1.0, wide[j])
        final = jnp.where(sub == j, base * lax.rsqrt(pivot), final)
        for i in range(j + 1, 8):
            scale = entry[i][j] * inverse
            wide[i] = jnp.where(here, 0.0, wide[i]) - scale * base
            for t in range(j + 1, i + 1):
                entry[i][t] = entry[i][t] - scale * entry[t][j]
    return final


def invert_factor(z_ref, middle):
    n = z_ref.shape[0]
    lane = lax.broadcasted_iota(jnp.int32, (8, n), 1)
    sub = lax.broadcasted_iota(jnp.int32, (8, n), 0)
    all_lane = lax.broadcasted_iota(jnp.int32, (n, n), 1)
    all_row = lax.broadcasted_iota(jnp.int32, (n, n), 0)

    def group(g, carry):
        first = pl.multiple_of(8 * g, 8)
        final = pivot_rows(z_ref[pl.ds(first, 8), :], lane, sub, first)
        right = jnp.where((lane < first + 8) & (lane > first + sub), 0.0, final)
        left = jnp.where(lane >= first + 8, final, 0.0)
        change = dot(left, right, 0, 0)
        mine = (all_lane >= first) & (all_lane < first + 8) & (all_row >= first + 8)
        z_ref[...] = jnp.where(mine, 0.0, z_ref[...]) - change
        z_ref[pl.ds(first, 8), :] = right
        return carry

    half = n // 16
    lax.fori_loop(0, half, group, 0)
    middle()
    lax.fori_loop(half, n // 8, group, 0)
    z_ref[...] = jnp.where(all_lane <= all_row, z_ref[...], 0.0)


def kernel(
    rows, cols, a_ref, o_ref, tiles, slab, blocks, work, inverse, w_ref,
    tile_send, tile_recv, slab_send, slab_recv,
):
    slots, size, _ = a_ref.shape
    half = size // 2
    r = lax.axis_index("row")
    c = lax.axis_index("col")
    bits = [k for k in range(rows.bit_length()) if (1 << k) < rows][::-1]

    def across(k):
        return r + (1 << k) * (1 - 2 * ((r // (1 << k)) % 2))

    barrier = pltpu.get_barrier_semaphore()
    for k in bits:
        pl.semaphore_signal(barrier, inc=1, device_id=(across(k), c), device_id_type=MESH)

    @pl.when(c > 0)
    def _():
        pl.semaphore_signal(barrier, inc=1, device_id=(r, c - 1), device_id_type=MESH)

    @pl.when(c < cols - 1)
    def _():
        pl.semaphore_signal(barrier, inc=1, device_id=(r, c + 1), device_id_type=MESH)

    peers = len(bits) + jnp.where(c > 0, 1, 0) + jnp.where(c < cols - 1, 1, 0)
    pl.semaphore_wait(barrier, peers)

    def place(t):
        root, owner_col, first_col, chunks = TILES[t]
        q = r if root == 0 else r + 1 - 2 * (r % 2)
        owner = (r == root) & ((c >= first_col) if owner_col is None else (c == owner_col))
        active = c >= first_col
        along = None
        if owner_col is not None:
            along = (r == root) & (c >= owner_col) & (c < cols - 1)
        down = [active & (q % (1 << (k + 1)) == 0) for k in bits]
        return chunks, owner, active & jnp.logical_not(owner), along, down

    def tile_copy(t, chunk, chunks, source, way, device):
        span = pl.ds(chunk * (size // chunks), size // chunks)
        return pltpu.make_async_remote_copy(
            src_ref=source.at[span],
            dst_ref=tiles.at[t, span],
            send_sem=tile_send.at[t, chunk, way],
            recv_sem=tile_recv.at[t, chunk],
            device_id=device,
            device_id_type=MESH,
        )

    def each_send(t, chunk, source, act):
        chunks, _, _, along, down = place(t)
        if along is not None:

            @pl.when(along)
            def _():
                act(tile_copy(t, chunk, chunks, source, 0, (r, c + 1)))

        for n, k in enumerate(bits):

            @pl.when(down[n])
            def _(n=n, k=k):
                act(tile_copy(t, chunk, chunks, source, n + 1, (across(k), c)))

    def slab_copy(which, s, source):
        return pltpu.make_async_remote_copy(
            src_ref=source.at[s],
            dst_ref=slab.at[which, s],
            send_sem=slab_send.at[which, s],
            recv_sem=slab_recv.at[which, s],
            device_id=(r, c + 1),
            device_id_type=MESH,
        )

    def needed(s):
        return (r >= 2) if s == 0 else (r >= 0)

    for t in range(len(TILES)):
        chunks, owner, _, _, _ = place(t)

        @pl.when(owner)
        def _(t=t, chunks=chunks):
            for chunk in range(chunks):
                each_send(t, chunk, a_ref.at[0], lambda copy: copy.start())

    def own_slab(which):
        for s in range(slots):

            @pl.when(needed(s))
            def _(s=s):
                slab_copy(which, s, a_ref).start()

    @pl.when(c == 0)
    def _():
        own_slab(0)

    if cols > 2:

        @pl.when((c == 1) & (r >= 2))
        def _():
            own_slab(1)

    for t in range(len(TILES)):

        @pl.when(place(t)[1])
        def _(t=t):
            tiles[t] = a_ref[0]

    for t in ARRIVAL:
        chunks, _, receives, _, _ = place(t)

        @pl.when(receives)
        def _(t=t, chunks=chunks):
            for chunk in range(chunks):
                tile_copy(t, chunk, chunks, tiles.at[t], 0, (r, c)).wait_recv()
                each_send(t, chunk, tiles.at[t], lambda copy: copy.start())

    if cols > 2:

        @pl.when((c == 1) & (r < 2))
        def _():
            own_slab(1)

    def pass_on(which, s):
        @pl.when(needed(s))
        def _():
            slab_copy(which, s, slab.at[which]).wait_recv()

            @pl.when(c < cols - 1)
            def _():
                slab_copy(which, s, slab.at[which]).start()

    def arrive(position):
        if position < slots:

            @pl.when(c == 1)
            def _():
                pass_on(0, position)

        @pl.when(c >= 2)
        def _():
            pass_on(1 if position < slots else 0, position % slots)

    pending = list(range(2 * slots))

    def take(count):
        for _ in range(min(count, len(pending))):
            arrive(pending.pop(0))

    def block_of(t, i, j):
        return tiles[t, i * half : (i + 1) * half, j * half : (j + 1) * half]

    def load(i, j):
        t = 0 if i < 2 else (1 if j < 2 else 2)
        blocks[i, j] = block_of(t, i % 2, j % 2)

    for i in range(2):
        for j in range(i + 1):
            load(i, j)

    @pl.when(c >= 1)
    def _():
        for i in range(2, 4):
            for j in range(i + 1):
                load(i, j)

    take(2)
    for k in range(4):
        def step(k=k):
            work[...] = blocks[k, k]
            invert_factor(work, lambda: None)

        if k < 2:
            step()
        else:
            pl.when(c >= 1)(step)
        take(1)

        def finish(k=k):
            m = work[...]
            for j in range(k):
                blocks[k, j] = dot(m, blocks[k, j])
            targets = range(k + 1, 4)
            scaled = {i: dot(blocks[i, k], m, 1, 1) for i in targets}
            for i in targets:
                for j in range(k):
                    blocks[i, j] = blocks[i, j] - dot(scaled[i], blocks[k, j])
                blocks[i, k] = -dot(scaled[i], m)
                for j in range(k + 1, i + 1):
                    blocks[i, j] = blocks[i, j] - dot(scaled[i], scaled[j], 1, 1)
            blocks[k, k] = m

        if k < 2:

            @pl.when(c == 0)
            def _(k=k):
                m = work[...]
                if k == 0:
                    scaled = dot(blocks[1, 0], m, 1, 1)
                    blocks[1, 0] = -dot(scaled, m)
                    blocks[1, 1] = blocks[1, 1] - dot(scaled, scaled, 1, 1)
                else:
                    blocks[1, 0] = dot(m, blocks[1, 0])
                blocks[k, k] = m

        pl.when(c >= 1)(finish)

    def gather(n, i, j, zero):
        for x in range(2):
            for y in range(2):
                span = (slice(x * half, (x + 1) * half), slice(y * half, (y + 1) * half))
                if zero and y > x:
                    inverse[(n,) + span] = jnp.zeros((half, half), F32)
                else:
                    inverse[(n,) + span] = blocks[2 * i + x, 2 * j + y]

    lower = lax.broadcasted_iota(jnp.int32, (size, size), 0) >= lax.broadcasted_iota(
        jnp.int32, (size, size), 1
    )
    gather(0, 0, 0, True)

    @pl.when(c >= 1)
    def _():
        gather(1, 1, 0, False)
        gather(2, 1, 1, True)

    @pl.when(c == 0)
    def _():
        for s in range(slots):
            o_ref[s] = dot(a_ref[s], inverse[0], 1, 1)

        @pl.when(r == 0)
        def _():
            o_ref[0] = jnp.where(lower, o_ref[0], 0.0)

    @pl.when(c == 1)
    def _():
        for s in range(slots):
            o_ref[s] = dot(a_ref[s], inverse[2], 1, 1)

        @pl.when(r == 1)
        def _():
            o_ref[0] = jnp.where(lower, o_ref[0] + dot(tiles[1], inverse[1], 1, 1), 0.0)

        @pl.when(r == 0)
        def _():
            o_ref[0] = jnp.zeros((size, size), F32)

    @pl.when(c >= 2)
    def _():
        top = dot(inverse[0], tiles[3])
        low = dot(inverse[1], tiles[3]) + dot(inverse[2], tiles[4])
        w_ref[0] = dot(inverse[0], top, 0, 0) + dot(inverse[1], low, 0, 0)
        w_ref[1] = dot(inverse[2], low, 0, 0)

        @pl.when(r < 2)
        def _():
            o_ref[0] = jnp.zeros((size, size), F32)

    done = 2 * slots - len(pending)
    for position in range(2 * slots):
        if position >= done:
            take(1)
        s = position % slots
        if position < slots:

            @pl.when((c == 1) & needed(s))
            def _(s=s):
                o_ref[s] = o_ref[s] + dot(slab[0, s], inverse[1], 1, 1)

            @pl.when((c >= 2) & needed(s))
            def _(s=s):
                o_ref[s] = a_ref[s] - dot(slab[1, s], w_ref[1])

        else:

            @pl.when((c >= 2) & needed(s))
            def _(s=s):
                o_ref[s] = o_ref[s] - dot(slab[0, s], w_ref[0])

    for t in range(len(TILES)):
        for chunk in range(TILES[t][3]):
            each_send(t, chunk, tiles.at[t], lambda copy: copy.wait_send())
    for s in range(slots):

        @pl.when(needed(s) & (c < cols - 1))
        def _(s=s):
            slab_copy(0, s, a_ref).wait_send()

        @pl.when(needed(s) & (c >= 1) & (c < cols - 1))
        def _(s=s):
            slab_copy(1, s, a_ref).wait_send()


def solution(mesh):
    rows, cols = mesh.shape["row"], mesh.shape["col"]
    ways = rows.bit_length() + 1

    def body(choi):
        slots, size, _ = choi.shape
        half = size // 2
        vmem = pl.BlockSpec(memory_space=pltpu.VMEM)
        return pl.pallas_call(
            functools.partial(kernel, rows, cols),
            out_shape=jax.ShapeDtypeStruct(choi.shape, F32),
            in_specs=[vmem],
            out_specs=vmem,
            scratch_shapes=[
                pltpu.VMEM((len(TILES), size, size), F32),
                pltpu.VMEM((2, slots, size, size), F32),
                pltpu.VMEM((4, 4, half, half), F32),
                pltpu.VMEM((half, half), F32),
                pltpu.VMEM((3, size, size), F32),
                pltpu.VMEM((2, size, size), F32),
                pltpu.SemaphoreType.DMA((len(TILES), MAX_CHUNKS, ways)),
                pltpu.SemaphoreType.DMA((len(TILES), MAX_CHUNKS)),
                pltpu.SemaphoreType.DMA((2, slots)),
                pltpu.SemaphoreType.DMA((2, slots)),
            ],
            compiler_params=pltpu.CompilerParams(collective_id=0, has_side_effects=True),
        )(choi)

    return jax.shard_map(
        body,
        mesh=mesh,
        in_specs=(P(None, "row", "col"),),
        out_specs=P(None, "row", "col"),
        check_vma=False,
    )
```

```python
import functools

import jax
import jax.numpy as jnp
from jax import lax
from jax.experimental import pallas as pl
from jax.experimental.pallas import tpu as pltpu
from jax.sharding import PartitionSpec as P

MESH = pl.DeviceIdType.MESH
HIGHEST = lax.Precision.HIGHEST
F32 = jnp.float32

TILES = ((0, 0, 0, 4), (1, 0, 1, 2), (1, 1, 1, 2), (0, None, 2, 2), (1, None, 2, 2))
MAX_CHUNKS = 4


def dot(a, b, ca=1, cb=0, precision=HIGHEST):
    return lax.dot_general(
        a, b, (((ca,), (cb,)), ((), ())), precision=precision, preferred_element_type=F32
    )


def split(x):
    high = x.astype(jnp.bfloat16)
    return high, (x - high.astype(F32)).astype(jnp.bfloat16)


def dot3(a, b):
    (ah, al), (bh, bl) = a, b

    def one(x, y):
        return jnp.dot(x, y, preferred_element_type=F32)

    return one(al, bh) + one(ah, bl) + one(ah, bh)


def pivot_rows(rows, lane, sub, first):
    n = rows.shape[1]
    wide = [jnp.broadcast_to(rows[j : j + 1, :], (8, n)) for j in range(8)]
    columns = [
        jnp.sum(jnp.where(lane == first + j, rows, 0.0), axis=1, keepdims=True) for j in range(8)
    ]
    columns = [jnp.broadcast_to(c, (8, n)) for c in columns]
    entry = [
        [jnp.broadcast_to(columns[j][i : i + 1, :], (8, n)) if j <= i else None for j in range(8)]
        for i in range(8)
    ]
    final = jnp.zeros((8, n), F32)
    for j in range(8):
        here = lane == first + j
        pivot = entry[j][j]
        inverse = 1.0 / pivot
        base = jnp.where(here, 1.0, wide[j])
        final = jnp.where(sub == j, base * lax.rsqrt(pivot), final)
        for i in range(j + 1, 8):
            scale = entry[i][j] * inverse
            wide[i] = jnp.where(here, 0.0, wide[i]) - scale * base
            for t in range(j + 1, i + 1):
                entry[i][t] = entry[i][t] - scale * entry[t][j]
    return final


def invert_factor(z_ref, between):
    n = z_ref.shape[0]
    lane = lax.broadcasted_iota(jnp.int32, (8, n), 1)
    sub = lax.broadcasted_iota(jnp.int32, (8, n), 0)
    all_lane = lax.broadcasted_iota(jnp.int32, (n, n), 1)
    all_row = lax.broadcasted_iota(jnp.int32, (n, n), 0)

    def group(g, carry):
        first = pl.multiple_of(8 * g, 8)
        final = pivot_rows(z_ref[pl.ds(first, 8), :], lane, sub, first)
        right = jnp.where((lane < first + 8) & (lane > first + sub), 0.0, final)
        left = jnp.where(lane >= first + 8, final, 0.0)
        change = dot(left, right, 0, 0)
        mine = (all_lane >= first) & (all_lane < first + 8) & (all_row >= first + 8)
        z_ref[...] = jnp.where(mine, 0.0, z_ref[...]) - change
        z_ref[pl.ds(first, 8), :] = right
        return carry

    quarter = n // 32
    for part in range(4):
        lax.fori_loop(part * quarter, (part + 1) * quarter, group, 0)
        between(part)
    z_ref[...] = jnp.where(all_lane <= all_row, z_ref[...], 0.0)


def kernel(
    rows, cols, a_ref, o_ref, tiles, slab, blocks, work, inverse, rhs, w_high, w_low,
    tile_send, tile_recv, slab_send, slab_recv,
):
    slots, size, _ = a_ref.shape
    half = size // 2
    r = lax.axis_index("row")
    c = lax.axis_index("col")
    bits = [k for k in range(rows.bit_length()) if (1 << k) < rows][::-1]

    def across(k):
        return r + (1 << k) * (1 - 2 * ((r // (1 << k)) % 2))

    barrier = pltpu.get_barrier_semaphore()
    for k in bits:
        pl.semaphore_signal(barrier, inc=1, device_id=(across(k), c), device_id_type=MESH)

    @pl.when(c > 0)
    def _():
        pl.semaphore_signal(barrier, inc=1, device_id=(r, c - 1), device_id_type=MESH)

    @pl.when(c < cols - 1)
    def _():
        pl.semaphore_signal(barrier, inc=1, device_id=(r, c + 1), device_id_type=MESH)

    peers = len(bits) + jnp.where(c > 0, 1, 0) + jnp.where(c < cols - 1, 1, 0)
    pl.semaphore_wait(barrier, peers)

    def place(t):
        root, owner_col, first_col, chunks = TILES[t]
        q = r if root == 0 else r + 1 - 2 * (r % 2)
        owner = (r == root) & ((c >= first_col) if owner_col is None else (c == owner_col))
        active = c >= first_col
        along = None
        if owner_col is not None:
            along = (r == root) & (c >= owner_col) & (c < cols - 1)
        down = [active & (q % (1 << (k + 1)) == 0) for k in bits]
        return chunks, owner, active & jnp.logical_not(owner), along, down

    def tile_copy(t, chunk, chunks, source, way, device):
        span = pl.ds(chunk * (size // chunks), size // chunks)
        return pltpu.make_async_remote_copy(
            src_ref=source.at[span],
            dst_ref=tiles.at[t, span],
            send_sem=tile_send.at[t, chunk, way],
            recv_sem=tile_recv.at[t, chunk],
            device_id=device,
            device_id_type=MESH,
        )

    def each_send(t, chunk, source, act):
        chunks, _, _, along, down = place(t)
        if along is not None:

            @pl.when(along)
            def _():
                act(tile_copy(t, chunk, chunks, source, 0, (r, c + 1)))

        for n, k in enumerate(bits):

            @pl.when(down[n])
            def _(n=n, k=k):
                act(tile_copy(t, chunk, chunks, source, n + 1, (across(k), c)))

    def slab_copy(which, s, source):
        return pltpu.make_async_remote_copy(
            src_ref=source.at[s],
            dst_ref=slab.at[which, s],
            send_sem=slab_send.at[which, s],
            recv_sem=slab_recv.at[which, s],
            device_id=(r, c + 1),
            device_id_type=MESH,
        )

    def needed(s):
        return (r >= 2) if s == 0 else (r >= 0)

    for t in range(len(TILES)):
        chunks, owner, _, _, _ = place(t)

        @pl.when(owner)
        def _(t=t, chunks=chunks):
            for chunk in range(chunks):
                each_send(t, chunk, a_ref.at[0], lambda copy: copy.start())

    def own_slab(which):
        for s in range(slots):

            @pl.when(needed(s))
            def _(s=s):
                slab_copy(which, s, a_ref).start()

    @pl.when(c == 0)
    def _():
        own_slab(0)

    if cols > 2:

        @pl.when((c == 1) & (r >= 2))
        def _():
            own_slab(1)

    for t in range(len(TILES)):

        @pl.when(place(t)[1])
        def _(t=t):
            tiles[t] = a_ref[0]

    def collect(t, which):
        chunks, _, receives, _, _ = place(t)

        @pl.when(receives & which)
        def _():
            for chunk in range(chunks):
                tile_copy(t, chunk, chunks, tiles.at[t], 0, (r, c)).wait_recv()
                each_send(t, chunk, tiles.at[t], lambda copy: copy.start())

    beyond = r + 1 - 2 * (r % 2)
    depth = sum((beyond // (1 << k)) % 2 for k in bits)
    for t in (3, 4, 0):
        collect(t, r >= 0)
    for t in (1, 2):
        collect(t, depth == 0)

    if cols > 2:

        @pl.when((c == 1) & (r < 2))
        def _():
            own_slab(1)

    def land(which, s):
        slab_copy(which, s, slab.at[which]).wait_recv()

    def pass_on(which, s):
        land(which, s)
        slab_copy(which, s, slab.at[which]).start()

    def arrive(position):
        s = position % slots
        which = 1 if position < slots else 0
        if position < slots:
            only = (c == 1) & needed(s)
            pl.when(only & (c < cols - 1))(lambda: pass_on(0, s))
            pl.when(only & (c == cols - 1))(lambda: land(0, s))
        if cols > 3:
            pl.when((c >= 2) & (c < cols - 1) & needed(s))(lambda: pass_on(which, s))

    pending = list(range(2 * slots))

    def take(count):
        for _ in range(min(count, len(pending))):
            arrive(pending.pop(0))

    def block_of(t, i, j):
        return tiles[t, i * half : (i + 1) * half, j * half : (j + 1) * half]

    for i in range(2):
        for j in range(i + 1):
            blocks[i, j] = block_of(0, i, j)

    @pl.when(c >= 1)
    def _():
        for i in range(2, 4):
            for j in range(2, i + 1):
                blocks[i, j] = jnp.zeros((half, half), F32)

    @pl.when(c >= 2)
    def _():
        for i in range(4):
            rhs[i] = tiles[3 + i // 2, (i % 2) * half : (i % 2 + 1) * half, :]

    during = ((1, 1), (1, 1), (0, 1), (1, 0))

    def between(k, part):
        if k == 0 and part == 0:
            collect(1, depth == 1)
        if k == 0 and part == 2:
            collect(1, depth == 2)
        if k == 0 and part == 3:
            collect(1, depth >= 3)
            collect(2, depth == 1)
        if k == 1 and part == 1:
            collect(2, depth == 2)
        if k == 1 and part == 3:
            collect(2, depth >= 3)
        if part == 1:
            take(during[k][0])

    take(2)
    for k in range(4):
        if k == 2:

            @pl.when(c >= 1)
            def _():
                for i in range(2, 4):
                    for j in range(2, i + 1):
                        blocks[i, j] = blocks[i, j] + block_of(2, i - 2, j - 2)

        def step(k=k):
            work[...] = blocks[k, k]
            invert_factor(work, lambda part: between(k, part))

        if k < 2:
            step()
        else:
            pl.when(c >= 1)(step)
        take(during[k][1])
        if k == 0:

            @pl.when(c >= 1)
            def _():
                for i in range(2, 4):
                    for j in range(2):
                        blocks[i, j] = block_of(1, i - 2, j)


        def finish(k=k):
            m = work[...]
            for j in range(k):
                blocks[k, j] = dot(m, blocks[k, j])
            targets = range(k + 1, 4)
            scaled = {i: dot(blocks[i, k], m, 1, 1) for i in targets}
            for i in targets:
                for j in range(k):
                    blocks[i, j] = blocks[i, j] - dot(scaled[i], blocks[k, j])
                blocks[i, k] = -dot(scaled[i], m)
                for j in range(k + 1, i + 1):
                    blocks[i, j] = blocks[i, j] - dot(scaled[i], scaled[j], 1, 1)
            blocks[k, k] = m

        if k < 2:

            @pl.when(c == 0)
            def _(k=k):
                m = work[...]
                if k == 0:
                    scaled = dot(blocks[1, 0], m, 1, 1)
                    blocks[1, 0] = -dot(scaled, m)
                    blocks[1, 1] = blocks[1, 1] - dot(scaled, scaled, 1, 1)
                else:
                    blocks[1, 0] = dot(m, blocks[1, 0])
                blocks[k, k] = m

        pl.when(c == 1)(finish)

        @pl.when(c >= 2)
        def _(k=k):
            m = work[...]
            scaled = {i: dot(blocks[i, k], m, 1, 1) for i in range(k + 1, 4)}
            for i in scaled:
                for j in range(k + 1, i + 1):
                    blocks[i, j] = blocks[i, j] - dot(scaled[i], scaled[j], 1, 1)
                blocks[i, k] = scaled[i]
            blocks[k, k] = m
            y = dot(m, rhs[k])
            for i in scaled:
                rhs[i] = rhs[i] - dot(scaled[i], y)
            rhs[k] = y

    def gather(n, i, j, zero):
        for x in range(2):
            for y in range(2):
                span = (slice(x * half, (x + 1) * half), slice(y * half, (y + 1) * half))
                if zero and y > x:
                    inverse[(n,) + span] = jnp.zeros((half, half), F32)
                else:
                    inverse[(n,) + span] = blocks[2 * i + x, 2 * j + y]

    lower = lax.broadcasted_iota(jnp.int32, (size, size), 0) >= lax.broadcasted_iota(
        jnp.int32, (size, size), 1
    )
    @pl.when(c == 0)
    def _():
        gather(0, 0, 0, True)

    @pl.when(c == 1)
    def _():
        gather(1, 1, 0, False)
        gather(2, 1, 1, True)

    @pl.when(c == 0)
    def _():
        for s in range(slots):
            o_ref[s] = dot(a_ref[s], inverse[0], 1, 1)

        @pl.when(r == 0)
        def _():
            o_ref[0] = jnp.where(lower, o_ref[0], 0.0)

    @pl.when(c == 1)
    def _():
        for s in range(slots):
            o_ref[s] = dot(a_ref[s], inverse[2], 1, 1)

        @pl.when(r == 1)
        def _():
            o_ref[0] = jnp.where(lower, o_ref[0] + dot(tiles[1], inverse[1], 1, 1), 0.0)

        @pl.when(r == 0)
        def _():
            o_ref[0] = jnp.zeros((size, size), F32)

    @pl.when(c >= 2)
    def _():
        w = {}
        for k in reversed(range(4)):
            x = rhs[k]
            for i in range(k + 1, 4):
                x = x - dot(blocks[i, k], w[i], 0, 0)
            w[k] = dot(blocks[k, k], x, 0, 0)
            high, low = split(w[k])
            span = slice((k % 2) * half, (k % 2 + 1) * half)
            w_high[k // 2, span, :] = high
            w_low[k // 2, span, :] = low

    @pl.when((c >= 2) & (r < 2))
    def _():
        o_ref[0] = a_ref[0]

    done = 2 * slots - len(pending)
    for position in range(2 * slots):
        if position >= done:
            take(1)
        s = position % slots
        if position < slots:

            @pl.when((c == 1) & needed(s))
            def _(s=s):
                o_ref[s] = o_ref[s] + dot(slab[0, s], inverse[1], 1, 1)

            @pl.when((c >= 2) & (c == cols - 1) & needed(s))
            def _(s=s):
                land(1, s)

            @pl.when((c >= 2) & needed(s))
            def _(s=s):
                o_ref[s] = a_ref[s] - dot3(split(slab[1, s]), (w_high[1], w_low[1]))

        else:

            @pl.when((c >= 2) & (c == cols - 1) & needed(s))
            def _(s=s):
                land(0, s)

            @pl.when((c >= 2) & needed(s))
            def _(s=s):
                o_ref[s] = o_ref[s] - dot3(split(slab[0, s]), (w_high[0], w_low[0]))

    for t in range(len(TILES)):
        for chunk in range(TILES[t][3]):
            each_send(t, chunk, tiles.at[t], lambda copy: copy.wait_send())
    for s in range(slots):

        @pl.when(needed(s) & (c < cols - 1))
        def _(s=s):
            slab_copy(0, s, a_ref).wait_send()

        @pl.when(needed(s) & (c >= 1) & (c < cols - 1))
        def _(s=s):
            slab_copy(1, s, a_ref).wait_send()


def solution(mesh):
    rows, cols = mesh.shape["row"], mesh.shape["col"]
    ways = rows.bit_length() + 1

    def body(choi):
        slots, size, _ = choi.shape
        half = size // 2
        vmem = pl.BlockSpec(memory_space=pltpu.VMEM)
        result = pl.pallas_call(
            functools.partial(kernel, rows, cols),
            out_shape=jax.ShapeDtypeStruct(choi.shape, F32),
            in_specs=[vmem],
            out_specs=vmem,
            scratch_shapes=[
                pltpu.VMEM((len(TILES), size, size), F32),
                pltpu.VMEM((2, slots, size, size), F32),
                pltpu.VMEM((4, 4, half, half), F32),
                pltpu.VMEM((half, half), F32),
                pltpu.VMEM((3, size, size), F32),
                pltpu.VMEM((4, half, size), F32),
                pltpu.VMEM((2, size, size), jnp.bfloat16),
                pltpu.VMEM((2, size, size), jnp.bfloat16),
                pltpu.SemaphoreType.DMA((len(TILES), MAX_CHUNKS, ways)),
                pltpu.SemaphoreType.DMA((len(TILES), MAX_CHUNKS)),
                pltpu.SemaphoreType.DMA((2, slots)),
                pltpu.SemaphoreType.DMA((2, slots)),
            ],
            compiler_params=pltpu.CompilerParams(collective_id=0, has_side_effects=True),
        )(choi)
        tile_row = jnp.arange(slots, dtype=jnp.int32) * rows + lax.axis_index("row")
        cleared = (lax.axis_index("col") >= 2) & (tile_row[:, None, None] < 2)
        return jnp.where(cleared, 0.0, result)

    return jax.shard_map(
        body,
        mesh=mesh,
        in_specs=(P(None, "row", "col"),),
        out_specs=P(None, "row", "col"),
        check_vma=False,
    )
```
